512 devices in a mesh: mem: 32 (over y, z_lo, core), row: 4 (over x), col: 4 (over z_hi).
Axes of the slice: x: 4, y: 8, z: 8 (z_hi: 4, z_lo: 2; z = z_hi * 2 + z_lo), core: 2. Of those that a mesh axis runs over, the one named last changes fastest.
Arguments:
- background_sample: float32 [64, 4, 32, 32, 512], P('mem', None, None, 'row', 'col'), may hold values from -6 to 6
- coupling: float32 [4, 4], replicated, may hold values from -0.6 to 0.6
- diffusion: float32 [32], replicated, may hold values from 0.02 to 0.12
- wind_row: float32 [32], replicated, may hold values from -0.4 to 0.4
- wind_col: float32 [32], replicated, may hold values from -0.4 to 0.4
- observed_entry_index: int32 [64, 32, 512], P(None, 'row', ('col', 'mem')), may hold values from 0 to 127
- obs_value: float32 [64, 32, 512], P(None, 'row', ('col', 'mem')), may hold values from -6 to 6
- obs_weight: float32 [64, 32, 512], P(None, 'row', ('col', 'mem')), may hold values from 0.25 to 4
Outputs:
- analysis: float32 [64, 4, 32, 32, 512], P(None, None, None, 'row', ('col', 'mem'))
The draws below stay inside these ranges and needn't reach their ends.
Inputs may be any that keep to these rules, and one draw needn't show every extreme that they name: observed_entry_index names an entry of a column as variable times 32 plus level.
All inputs are finite; a program needn't handle non-finite values.
Results may differ from the reference program's by a relative error of at most 0.0003.
Values sent between devices are 32-bit elements; how exact they have to be, the bound alone decides.
No kernel may reach another device: no remote copies, remote signals or barrier semaphores. Data moves between devices by JAX's collectives and lax.ppermute only.
A program may use at most 64 MiB of HBM per device.

```python
import math
import jax
import jax.numpy as jnp
from jax import lax

MEM = 64
V = 4
L = 32
K = 64
STEPS = 2
NS_ITERS = 2
NR = 32
NC = 512


def place_ends(values, rng, least, largest):
    longest = values.shape.index(max(values.shape))
    spots = []
    for shift in (0, 1):
        where = [jax.random.randint(jax.random.fold_in(rng, axis), (), 0, length) for axis, length in enumerate(values.shape)]
        where[longest] = (where[longest] + shift) % values.shape[longest]
        spots.append(tuple(where))
    return values.at[spots[0]].set(least).at[spots[1]].set(largest)


def block_levels(stream_key, dims, split, smallest, top_value):
    level, own = 1.0, jax.random.fold_in(stream_key, 6)
    for axis_at, shards_of in split:
        heights = jnp.exp(jax.random.uniform(jax.random.fold_in(own, axis_at), (shards_of,), jnp.float32, smallest / len(split), top_value / len(split)))
        level = level * jnp.repeat(heights, dims[axis_at] // shards_of).reshape([-1 if axis == axis_at else 1 for axis in range(len(dims))])
    return level


def gaussian(rng, shape, width, bound, pieces=(), held_as=jnp.bfloat16):
    values = width * jax.random.normal(rng, shape, jnp.float32)
    if pieces:
        values = values * block_levels(rng, shape, pieces, -0.22, 0.18)
    return jnp.clip(values, -bound, bound).astype(held_as)


def setup_inputs(seed: int = 0) -> dict:
    streams_of = jax.random.split(jax.random.key(seed), 9)
    background_sample = gaussian(streams_of[0], (MEM, V, L, NR, NC), 1.0, 6.0, ((0, 32), (3, 4), (4, 4)), jnp.float32)
    coupling = gaussian(streams_of[1], (V, V), 0.15, 0.6, (), jnp.float32)
    diffusion = jnp.clip(jax.random.uniform(streams_of[2], (L,), jnp.float32, 0.02, 0.12), 0.02, 0.12)
    wind_row = jnp.clip(jax.random.uniform(streams_of[3], (L,), jnp.float32, -0.4, 0.4), -0.4, 0.4)
    wind_col = jnp.clip(jax.random.uniform(streams_of[4], (L,), jnp.float32, -0.4, 0.4), -0.4, 0.4)
    observed_entry_index = place_ends(jax.random.randint(streams_of[5], (K, NR, NC), 0, V * L), jax.random.fold_in(streams_of[5], 1), 0, (V * L) - 1).astype(jnp.int32)
    obs_value = gaussian(streams_of[6], (K, NR, NC), 1.0, 6.0, ((1, 4), (2, 128)), jnp.float32)
    obs_weight = jnp.clip(jnp.exp(math.log(4.0) - 2.7725887 * jax.random.uniform(streams_of[7], (K, NR, NC), jnp.float32) ** block_levels(streams_of[7], (K, NR, NC), ((1, 4), (2, 128)), -0.2, 0.2)), 0.25, 4.0)
    return {"background_sample": background_sample, "coupling": coupling, "diffusion": diffusion, "wind_row": wind_row, "wind_col": wind_col, "observed_entry_index": observed_entry_index, "obs_value": obs_value, "obs_weight": obs_weight}


def tendency(padded, diffusion, wind_row, wind_col, coupling):
    centre = padded[..., 1:-1, 1:-1]
    north = padded[..., :-2, 1:-1]
    south = padded[..., 2:, 1:-1]
    west = padded[..., 1:-1, :-2]
    east = padded[..., 1:-1, 2:]
    ensemble_spread = north + south + west + east - 4.0 * centre
    mixed = jnp.einsum('vw,...wlij->...vlij', coupling, centre, precision=lax.Precision.HIGHEST)
    return diffusion[:, None, None] * ensemble_spread - 0.5 * wind_row[:, None, None] * (south - north) - 0.5 * wind_col[:, None, None] * (east - west) + mixed

def bordered(field):
    return jnp.pad(field, ((0, 0), (0, 0), (1, 1), (1, 1)))

def analyse(block, index, value, weight):
    members = block.shape[0]
    entries = block.shape[1]
    highest = lax.Precision.HIGHEST
    mean = lax.optimization_barrier(jnp.mean(block, axis=0))
    pert = block - mean[None]
    onehot = (index[:, None, :] == jnp.arange(entries, dtype=jnp.int32)[None, :, None]).astype(jnp.float32)
    measurement_data = jnp.einsum('mvc,kvc->mkc', block, onehot, precision=highest)
    obs_mean = lax.optimization_barrier(jnp.mean(measurement_data, axis=0))
    obs_pert = measurement_data - obs_mean[None]
    scaled = obs_pert * weight[None]
    eye = jnp.eye(members, dtype=jnp.float32)[:, :, None]
    system = jnp.einsum('mkc,nkc->mnc', scaled, obs_pert, precision=highest) + (members - 1.0) * eye
    scale = jnp.sqrt(lax.optimization_barrier(jnp.sum(system * system, axis=(0, 1))))
    current = system / scale[None, None]
    inverse = jnp.broadcast_to(eye, system.shape)
    for sweep in range(NS_ITERS):
        factor = 1.5 * eye - 0.5 * jnp.einsum('mjc,jnc->mnc', inverse, current, precision=highest)
        current = jnp.einsum('mjc,jnc->mnc', current, factor, precision=highest)
        inverse = jnp.einsum('mjc,jnc->mnc', factor, inverse, precision=highest)
    gain_vec = jnp.einsum('mkc,kc->mc', scaled, value - obs_mean, precision=highest)
    half_vec = jnp.einsum('mjc,jc->mc', inverse, gain_vec, precision=highest)
    centre = jnp.einsum('mjc,jc->mc', inverse, half_vec, precision=highest) / scale[None]
    analysis_coefficients = inverse * jnp.sqrt((members - 1.0) / scale)[None, None] + centre[:, None, :]
    return mean[None] + jnp.einsum('mvc,mnc->nvc', pert, analysis_coefficients, precision=highest)

def reference(background_sample, coupling, diffusion, wind_row, wind_col, observed_entry_index, obs_value, obs_weight):

    def background_prediction(sample_number):
        state = sample_number
        for step in range(STEPS):
            first = tendency(bordered(state), diffusion, wind_row, wind_col, coupling)
            middle = state + first
            second = tendency(bordered(middle), diffusion, wind_row, wind_col, coupling)
            state = state + 0.5 * (first + second)
        return state
    sample_fields = lax.map(background_prediction, background_sample)
    members = sample_fields.shape[0]
    flat = sample_fields.reshape(members, V * L, NR, NC)

    def per_row(row_number):
        block = lax.dynamic_index_in_dim(flat, row_number, 2, keepdims=False)
        index = lax.dynamic_index_in_dim(observed_entry_index, row_number, 1, keepdims=False)
        value = lax.dynamic_index_in_dim(obs_value, row_number, 1, keepdims=False)
        weight = lax.dynamic_index_in_dim(obs_weight, row_number, 1, keepdims=False)
        return analyse(block, index, value, weight)
    result = lax.map(per_row, jnp.arange(NR, dtype=jnp.int32))
    return jnp.moveaxis(result, 0, 2).reshape(members, V, L, NR, NC)
```

```python
import jax
import jax.numpy as jnp
from jax import lax
from jax.experimental import pallas as pl
from jax.experimental.pallas import tpu as pltpu
from jax.sharding import PartitionSpec as P

HALO = 4
EDGE = 16
DEPTH = (14, 12, 10, 8)
GROUP = 4
GRANT = pltpu.CompilerParams(vmem_limit_bytes=14 * 2**20)
NEWTON = (2.25, -2.4375, 1.6875, -0.5625, 0.0625)


def turn_kernel(block, top, bottom, west, east):
    members, entries, rows, cols = block.shape
    flat = block.reshape(members, entries * rows, cols)
    for m in range(members):
        for i in range(rows):
            plane = flat[m, pl.ds(i, entries, stride=rows), :].T
            half = top if i < HALO else bottom
            half[m, i % HALO] = plane
            west[m, i] = plane[:HALO]
            east[m, i] = plane[cols - HALO :]


def turn(block):
    members, variables, levels, rows, cols = block.shape
    entries = variables * levels
    half = jax.ShapeDtypeStruct((members, HALO, cols, entries), jnp.float32)
    side = jax.ShapeDtypeStruct((members, rows, HALO, entries), jnp.float32)
    return pl.pallas_call(
        turn_kernel,
        out_shape=[half, half, side, side],
        compiler_params=GRANT,
        name="turn",
    )(block.reshape(members, entries, rows, cols))


def forecast_kernel(
    coupling, rates, top, bottom, north, south, west, east, corner_n, corner_s, out, state, slope, mixer
):
    members, _, cols, entries = top.shape
    dests, listed, _ = out.shape
    cells = listed // members
    variables = coupling.shape[0]
    levels = entries // variables
    share = cols // dests
    rows = 2 * HALO
    last = EDGE + cols
    inside = [
        jnp.where(test, 1.0, 0.0)
        for test in (
            lax.axis_index("row") > 0,
            lax.axis_index("row") < lax.axis_size("row") - 1,
            lax.axis_index("col") > 0,
            lax.axis_index("col") < lax.axis_size("col") - 1,
        )
    ]
    diffusion, wind_row, wind_col = (
        jnp.concatenate([rates[k : k + 1]] * variables, axis=1) for k in range(3)
    )
    c_n, c_s = (diffusion + 0.5 * wind_row, diffusion - 0.5 * wind_row)
    c_w, c_e = (diffusion + 0.5 * wind_col, diffusion - 0.5 * wind_col)
    source = lax.broadcasted_iota(jnp.int32, (entries, entries), 0)
    target = lax.broadcasted_iota(jnp.int32, (entries, entries), 1)
    mixing = jnp.where(source == target, -4.0 * diffusion, 0.0)
    for v in range(variables):
        for w in range(variables):
            hit = (target - source == levels * (v - w)) & (target // levels == v)
            mixing += jnp.where(hit, coupling[v, w], 0.0)
    mixer[...] = jnp.concatenate([jnp.concatenate(halves(mixing), axis=1)] * 2, axis=0)

    def tendency(field, i, deep, start, size):
        here = field[pl.ds(i, deep), pl.ds(start, size), :]
        parts = jnp.concatenate(halves(here), axis=2).reshape(deep * size, 2 * entries)
        both = lax.dot_general(
            parts, mixer[...], (((1,), (0,)), ((), ())), preferred_element_type=jnp.float32
        )
        total = c_n * field[pl.ds(i - 1, deep), pl.ds(start, size), :]
        total += c_s * field[pl.ds(i + 1, deep), pl.ds(start, size), :]
        total += c_w * field[pl.ds(i, deep), pl.ds(start - 1, size), :]
        total += c_e * field[pl.ds(i, deep), pl.ds(start + 1, size), :]
        both = both.reshape(deep, size, 2 * entries)
        return here, total + (both[:, :, :entries] + both[:, :, entries:])

    def masked(value, i):
        deep, size, _ = value.shape
        row = i + lax.broadcasted_iota(jnp.int32, (deep, 1, 1), 0)
        value = value * jnp.where(row < HALO, inside[0], jnp.where(row >= 3 * HALO, inside[1], 1.0))
        where = first + lax.broadcasted_iota(jnp.int32, (1, size, 1), 1)
        return value * jnp.where(where < EDGE, inside[2], jnp.where(where >= last, inside[3], 1.0))

    first, wide = (EDGE - 8, cols + 16)

    def rates_of(low, high, deep):
        def step(b, carry):
            i = low + deep * b
            here, total = tendency(state, i, deep, first, wide)
            slope[pl.ds(i, deep), pl.ds(first, wide), :] = masked(total, i)
            return carry

        lax.fori_loop(0, (high - low) // deep, step, 0)

    def update(low, high, deep):
        def step(b, carry):
            i = low + deep * b
            here, total = tendency(slope, i, deep, first, wide)
            new = state[pl.ds(i, deep), pl.ds(first, wide), :] + here + 0.5 * total
            state[pl.ds(i, deep), pl.ds(first, wide), :] = masked(new, i)
            return carry

        lax.fori_loop(0, (high - low) // deep, step, 0)

    def member(m, carry):
        for i in range(HALO):
            state[i, EDGE:last] = north[m, i]
            state[HALO + i, EDGE:last] = top[m, i]
            state[2 * HALO + i, EDGE:last] = bottom[m, i]
            state[3 * HALO + i, EDGE:last] = south[m, i]
            state[i, EDGE - HALO : EDGE] = corner_n[m, i, :HALO]
            state[i, last : last + HALO] = corner_n[m, i, HALO:]
            state[3 * HALO + i, EDGE - HALO : EDGE] = corner_s[m, i, :HALO]
            state[3 * HALO + i, last : last + HALO] = corner_s[m, i, HALO:]
        for i in range(rows):
            state[HALO + i, EDGE - HALO : EDGE] = west[m, i]
            state[HALO + i, last : last + HALO] = east[m, i]
        rates_of(1, 15, DEPTH[0])
        update(2, 14, DEPTH[1])
        rates_of(3, 13, DEPTH[2])
        for i in range(0, rows, DEPTH[3]):
            here, total = tendency(slope, HALO + i, DEPTH[3], EDGE, cols)
            new = state[HALO + i : HALO + i + DEPTH[3], EDGE:last] + here + 0.5 * total
            for r in range(DEPTH[3]):
                for d in range(dests):
                    out[d, pl.ds(m * cells + (i + r) * share, share), :] = new[r, d * share : (d + 1) * share]
        return carry

    lax.fori_loop(0, members, member, 0)


def forecast(coupling, rates, top, bottom, north, south, west, east, corner_n, corner_s, dests):
    members, _, cols, entries = top.shape
    cells = 2 * HALO * cols // dests
    return pl.pallas_call(
        forecast_kernel,
        in_specs=[pl.BlockSpec(memory_space=pltpu.SMEM)] + [pl.BlockSpec()] * 9,
        out_shape=jax.ShapeDtypeStruct((dests, members * cells, entries), jnp.float32),
        scratch_shapes=[pltpu.VMEM((4 * HALO, cols + 2 * EDGE, entries), jnp.float32)] * 2
        + [pltpu.VMEM((2 * entries, 2 * entries), jnp.bfloat16)],
        compiler_params=GRANT,
        name="forecast",
    )(coupling, rates, top, bottom, north, south, west, east, corner_n, corner_s)


def weigh_kernel(index, value, weight, total, pulled):
    cells, observations = index.shape
    entries = total.shape[1]
    entry = lax.broadcasted_iota(jnp.int32, (cells, entries), 1)
    w = weight[...]
    wv = w * value[...]
    acc = jnp.zeros((cells, entries), jnp.float32)
    acc_v = jnp.zeros((cells, entries), jnp.float32)
    named = index[...]
    for k in range(observations):
        hit = jnp.broadcast_to(named[:, k : k + 1], (cells, entries)) == entry
        acc += jnp.where(hit, jnp.broadcast_to(w[:, k : k + 1], (cells, entries)), 0.0)
        acc_v += jnp.where(hit, jnp.broadcast_to(wv[:, k : k + 1], (cells, entries)), 0.0)
    total[...] = acc
    pulled[...] = acc_v


def weigh(index, value, weight, entries):
    shape = jax.ShapeDtypeStruct((index.shape[0], entries), jnp.float32)
    return pl.pallas_call(weigh_kernel, out_shape=[shape, shape], compiler_params=GRANT, name="weigh")(
        index, value, weight
    )


def halves(value):
    high = value.astype(jnp.bfloat16)
    return high, (value - high.astype(jnp.float32)).astype(jnp.bfloat16)


def product(a, b, turned=False):
    (ah, al), (bh, bl) = (a, b)
    dot = lambda u, v: lax.dot_general(
        u, v, (((1,), (1 if turned else 0,)), ((), ())), preferred_element_type=jnp.float32
    )
    both = dot(jnp.concatenate([ah, ah], axis=1), jnp.concatenate([bh, bl], axis=1 if turned else 0))
    return both + dot(al, bh)


def analyse_kernel(block, total, pulled, out):
    cells = total.shape[0]
    members = block.shape[0] // cells
    entries = block.shape[1]
    pair = 2 * members
    row_id = lax.broadcasted_iota(jnp.int32, (pair, pair), 0)
    col_id = lax.broadcasted_iota(jnp.int32, (pair, pair), 1)
    eye = (row_id == col_id).astype(jnp.float32)
    same = ((row_id < members) == (col_id < members)).astype(jnp.float32)
    left = lax.broadcasted_iota(jnp.int32, (1, pair), 1) < members
    n0, n1, n2, n3, n4 = NEWTON
    spread = lambda row: jnp.broadcast_to(row, (members, entries))

    def first(cell):
        x = [block[pl.ds(cell + u, members, stride=cells), :] for u in range(2)]
        mean = [jnp.sum(v, axis=0, keepdims=True) * (1.0 / members) for v in x]
        weight = [total[pl.ds(cell + u, 1), :] for u in range(2)]
        pull = [pulled[pl.ds(cell + u, 1), :] - mean[u] * weight[u] for u in range(2)]
        pert = [x[u] - mean[u] for u in range(2)]
        scaled = jnp.concatenate([pert[u] * weight[u] for u in range(2)], axis=0)
        gain = jnp.concatenate(
            [jnp.sum(pert[u] * pull[u], axis=1, keepdims=True) for u in range(2)], axis=0
        )
        system = product(halves(scaled), halves(jnp.concatenate(pert, axis=0)), turned=True)
        return jnp.concatenate(x, axis=0).T, gain, system * same + (members - 1.0) * eye

    def second(state):
        x_turned, gain, system = state
        square = jnp.sum(system * system, axis=0, keepdims=True)
        halved = [
            jnp.sum(jnp.where(side, square, 0.0), axis=1, keepdims=True) for side in (left, ~left)
        ]
        scale_inv = lax.rsqrt(jnp.where(left, halved[0], halved[1]))
        a = system * scale_inv
        parts = halves(a)
        return x_turned, gain, scale_inv, a, product(parts, parts)

    def third(state):
        x_turned, gain, scale_inv, a, b = state
        inverse = n0 * eye + n1 * a + n2 * b + product(halves(b), halves(n3 * a + n4 * b))
        return x_turned, gain, scale_inv, inverse

    def fourth(state):
        x_turned, gain, scale_inv, inverse = state
        half_vec = jnp.sum(inverse * gain, axis=0, keepdims=True)
        centre = jnp.sum(inverse * half_vec, axis=1, keepdims=True)
        weights = inverse * jnp.sqrt((members - 1.0) * scale_inv) + centre * (same * scale_inv)
        rest = (1.0 - jnp.sum(weights, axis=0, keepdims=True)) * (1.0 / members)
        return product(halves(x_turned), halves(weights + rest * same))

    def step(g, carry):
        cell = [g * (2 * GROUP) + 2 * u for u in range(GROUP)]
        states = [first(c) for c in cell]
        states = [second(s) for s in states]
        states = [third(s) for s in states]
        results = [fourth(s) for s in states]
        for c, result in zip(cell, results):
            out[pl.ds(c, entries, stride=cells), :] = result[:, :members]
            out[pl.ds(c + 1, entries, stride=cells), :] = result[:, members:]
        return carry

    lax.fori_loop(0, cells // (2 * GROUP), step, 0)


def analyse(block, total, pulled):
    cells, entries = total.shape
    members = block.shape[0] // cells
    return pl.pallas_call(
        analyse_kernel,
        out_shape=jax.ShapeDtypeStruct((entries * cells, members), jnp.float32),
        compiler_params=GRANT,
        name="analyse",
    )(block, total, pulled)


def neighbours(axis):
    up = [(i, i + 1) for i in range(lax.axis_size(axis) - 1)]
    return up, [(j, i) for i, j in up]


def body(
    background_sample,
    coupling,
    diffusion,
    wind_row,
    wind_col,
    observed_entry_index,
    obs_value,
    obs_weight,
):
    members_here, variables, levels, rows, cols = background_sample.shape
    entries = variables * levels
    dests = lax.axis_size("mem")
    top, bottom, own_w, own_e = turn(background_sample)
    col_up, col_down = neighbours("col")
    row_up, row_down = neighbours("row")
    west = lax.ppermute(own_e, "col", col_up)
    east = lax.ppermute(own_w, "col", col_down)
    north = lax.ppermute(bottom, "row", row_up)
    south = lax.ppermute(top, "row", row_down)
    sides = jnp.concatenate([west, east], axis=2)
    corner_n = lax.ppermute(sides[:, HALO:], "row", row_up)
    corner_s = lax.ppermute(sides[:, :HALO], "row", row_down)

    rates = jnp.stack([diffusion, wind_row, wind_col])
    sent = forecast(
        coupling, rates, top, bottom, north, south, west, east, corner_n, corner_s, dests
    )
    moved = lax.all_to_all(sent, "mem", split_axis=0, concat_axis=0, tiled=True)
    cells = rows * cols // dests
    members = dests * members_here

    def listed(x):
        return jnp.transpose(x, (1, 2, 0)).reshape(cells, x.shape[0])

    total, pulled = weigh(
        listed(observed_entry_index), listed(obs_value), listed(obs_weight), entries
    )
    result = analyse(moved.reshape(members * cells, entries), total, pulled)
    result = result.reshape(variables, levels, rows, cols // dests, members)
    return jnp.transpose(result, (4, 0, 1, 2, 3))


def solution(mesh):
    obs = P(None, "row", ("col", "mem"))
    return jax.shard_map(
        body,
        mesh=mesh,
        in_specs=(P("mem", None, None, "row", "col"), P(), P(), P(), P(), obs, obs, obs),
        out_specs=P(None, None, None, "row", ("col", "mem")),
        check_vma=False,
    )
```

```python
import jax
import jax.numpy as jnp
from jax import lax
from jax.experimental import pallas as pl
from jax.experimental.pallas import tpu as pltpu
from jax.sharding import PartitionSpec as P


HALO = 4
EDGE = 16
DEPTH = (14, 12, 10, 8)
GROUP = 4
GRANT = pltpu.CompilerParams(vmem_limit_bytes=14 * 2**20)
NEWTON = (2.25, -2.4375, 1.6875, -0.5625, 0.0625)


def turn_kernel(block, top, bottom, west, east, *corners):
    members, entries, rows, cols = block.shape
    flat = block.reshape(members, entries * rows, cols)
    for m in range(members):
        for i in range(rows):
            plane = flat[m, pl.ds(i, entries, stride=rows), :].T
            half = top if i < HALO else bottom
            half[m, i % HALO] = plane
            west[m, i] = plane[:HALO]
            east[m, i] = plane[cols - HALO :]
            pick = 0 if i < HALO else 2
            corners[pick][m, i % HALO] = plane[:HALO]
            corners[pick + 1][m, i % HALO] = plane[cols - HALO :]


def turn(block):
    members, variables, levels, rows, cols = block.shape
    entries = variables * levels
    half = jax.ShapeDtypeStruct((members, HALO, cols, entries), jnp.float32)
    side = jax.ShapeDtypeStruct((members, rows, HALO, entries), jnp.float32)
    corner = jax.ShapeDtypeStruct((members, HALO, HALO, entries), jnp.float32)
    return pl.pallas_call(
        turn_kernel,
        out_shape=[half, half, side, side] + [corner] * 4,
        compiler_params=GRANT,
        name="turn",
    )(block.reshape(members, entries, rows, cols))


def forecast_kernel(
    rates, top, bottom, north, south, west, east, nw, ne, sw, se, out, state, slope, mixer
):
    members, _, cols, entries = top.shape
    dests, listed, _ = out.shape
    cells = listed // members
    levels = rates.shape[1]
    variables = entries // levels
    share = cols // dests
    rows = 2 * HALO
    last = EDGE + cols
    inside = [
        jnp.where(test, 1.0, 0.0)
        for test in (
            lax.axis_index("row") > 0,
            lax.axis_index("row") < lax.axis_size("row") - 1,
            lax.axis_index("col") > 0,
            lax.axis_index("col") < lax.axis_size("col") - 1,
        )
    ]
    diffusion, wind_row, wind_col = (
        jnp.concatenate([rates[k : k + 1]] * variables, axis=1) for k in range(3)
    )
    c_n, c_s = (diffusion + 0.5 * wind_row, diffusion - 0.5 * wind_row)
    c_w, c_e = (diffusion + 0.5 * wind_col, diffusion - 0.5 * wind_col)
    source = lax.broadcasted_iota(jnp.int32, (entries, entries), 0)
    target = lax.broadcasted_iota(jnp.int32, (entries, entries), 1)
    mixing = jnp.where(source == target, -4.0 * diffusion, 0.0)
    for v in range(variables):
        for w in range(variables):
            hit = (target - source == levels * (v - w)) & (target // levels == v)
            mixing += jnp.where(hit, rates[3 + v : 4 + v, w : w + 1], 0.0)
    mixer[...] = jnp.concatenate([jnp.concatenate(halves(mixing), axis=1)] * 2, axis=0)

    def tendency(field, i, deep, start, size):
        here = field[pl.ds(i, deep), pl.ds(start, size), :]
        parts = jnp.concatenate(halves(here), axis=2).reshape(deep * size, 2 * entries)
        both = lax.dot_general(
            parts, mixer[...], (((1,), (0,)), ((), ())), preferred_element_type=jnp.float32
        )
        total = c_n * field[pl.ds(i - 1, deep), pl.ds(start, size), :]
        total += c_s * field[pl.ds(i + 1, deep), pl.ds(start, size), :]
        total += c_w * field[pl.ds(i, deep), pl.ds(start - 1, size), :]
        total += c_e * field[pl.ds(i, deep), pl.ds(start + 1, size), :]
        both = both.reshape(deep, size, 2 * entries)
        return here, total + (both[:, :, :entries] + both[:, :, entries:])

    def masked(value, i):
        deep, size, _ = value.shape
        row = i + lax.broadcasted_iota(jnp.int32, (deep, 1, 1), 0)
        value = value * jnp.where(row < HALO, inside[0], jnp.where(row >= 3 * HALO, inside[1], 1.0))
        where = first + lax.broadcasted_iota(jnp.int32, (1, size, 1), 1)
        return value * jnp.where(where < EDGE, inside[2], jnp.where(where >= last, inside[3], 1.0))

    first, wide = (EDGE - 8, cols + 16)

    def rates_of(low, high, deep):
        def step(b, carry):
            i = low + deep * b
            here, total = tendency(state, i, deep, first, wide)
            slope[pl.ds(i, deep), pl.ds(first, wide), :] = masked(total, i)
            return carry

        lax.fori_loop(0, (high - low) // deep, step, 0)

    def update(low, high, deep):
        def step(b, carry):
            i = low + deep * b
            here, total = tendency(slope, i, deep, first, wide)
            new = state[pl.ds(i, deep), pl.ds(first, wide), :] + here + 0.5 * total
            state[pl.ds(i, deep), pl.ds(first, wide), :] = masked(new, i)
            return carry

        lax.fori_loop(0, (high - low) // deep, step, 0)

    def member(m, carry):
        for i in range(HALO):
            state[i, EDGE:last] = north[m, i]
            state[HALO + i, EDGE:last] = top[m, i]
            state[2 * HALO + i, EDGE:last] = bottom[m, i]
            state[3 * HALO + i, EDGE:last] = south[m, i]
            state[i, EDGE - HALO : EDGE] = nw[m, i]
            state[i, last : last + HALO] = ne[m, i]
            state[3 * HALO + i, EDGE - HALO : EDGE] = sw[m, i]
            state[3 * HALO + i, last : last + HALO] = se[m, i]
        for i in range(rows):
            state[HALO + i, EDGE - HALO : EDGE] = west[m, i]
            state[HALO + i, last : last + HALO] = east[m, i]
        rates_of(1, 15, DEPTH[0])
        update(2, 14, DEPTH[1])
        rates_of(3, 13, DEPTH[2])
        for i in range(0, rows, DEPTH[3]):
            here, total = tendency(slope, HALO + i, DEPTH[3], EDGE, cols)
            new = state[HALO + i : HALO + i + DEPTH[3], EDGE:last] + here + 0.5 * total
            for r in range(DEPTH[3]):
                for d in range(dests):
                    out[d, pl.ds(m * cells + (i + r) * share, share), :] = new[r, d * share : (d + 1) * share]
        return carry

    lax.fori_loop(0, members, member, 0)


def forecast(dests, *operands):
    members, _, cols, entries = operands[1].shape
    cells = 2 * HALO * cols // dests
    return pl.pallas_call(
        forecast_kernel,
        out_shape=jax.ShapeDtypeStruct((dests, members * cells, entries), jnp.float32),
        scratch_shapes=[pltpu.VMEM((4 * HALO, cols + 2 * EDGE, entries), jnp.float32)] * 2
        + [pltpu.VMEM((2 * entries, 2 * entries), jnp.bfloat16)],
        compiler_params=GRANT,
        name="forecast",
    )(*operands)


def weigh_kernel(index, value, weight, total, pulled):
    cells, observations = index.shape
    entries = total.shape[1]
    entry = lax.broadcasted_iota(jnp.int32, (cells, entries), 1)
    w = weight[...]
    wv = w * value[...]
    acc = jnp.zeros((cells, entries), jnp.float32)
    acc_v = jnp.zeros((cells, entries), jnp.float32)
    named = index[...]
    for k in range(observations):
        hit = jnp.broadcast_to(named[:, k : k + 1], (cells, entries)) == entry
        acc += jnp.where(hit, jnp.broadcast_to(w[:, k : k + 1], (cells, entries)), 0.0)
        acc_v += jnp.where(hit, jnp.broadcast_to(wv[:, k : k + 1], (cells, entries)), 0.0)
    total[...] = acc
    pulled[...] = acc_v


def weigh(index, value, weight, entries):
    shape = jax.ShapeDtypeStruct((index.shape[0], entries), jnp.float32)
    return pl.pallas_call(weigh_kernel, out_shape=[shape, shape], compiler_params=GRANT, name="weigh")(
        index, value, weight
    )


def halves(value):
    high = value.astype(jnp.bfloat16)
    return high, (value - high.astype(jnp.float32)).astype(jnp.bfloat16)


def product(a, b, turned=False):
    (ah, al), (bh, bl) = (a, b)
    dot = lambda u, v: lax.dot_general(
        u, v, (((1,), (1 if turned else 0,)), ((), ())), preferred_element_type=jnp.float32
    )
    both = dot(jnp.concatenate([ah, ah], axis=1), jnp.concatenate([bh, bl], axis=1 if turned else 0))
    return both + dot(al, bh)


def analyse_kernel(block, total, pulled, out):
    cells = total.shape[0]
    members = block.shape[0] // cells
    entries = block.shape[1]
    pair = 2 * members
    row_id = lax.broadcasted_iota(jnp.int32, (pair, pair), 0)
    col_id = lax.broadcasted_iota(jnp.int32, (pair, pair), 1)
    eye = (row_id == col_id).astype(jnp.float32)
    same = ((row_id < members) == (col_id < members)).astype(jnp.float32)
    left = lax.broadcasted_iota(jnp.int32, (1, pair), 1) < members
    n0, n1, n2, n3, n4 = NEWTON
    spread = lambda row: jnp.broadcast_to(row, (members, entries))

    def first(cell):
        x = [block[pl.ds(cell + u, members, stride=cells), :] for u in range(2)]
        mean = [jnp.sum(v, axis=0, keepdims=True) * (1.0 / members) for v in x]
        weight = [total[pl.ds(cell + u, 1), :] for u in range(2)]
        pull = [pulled[pl.ds(cell + u, 1), :] - mean[u] * weight[u] for u in range(2)]
        pert = [x[u] - mean[u] for u in range(2)]
        scaled = jnp.concatenate([pert[u] * weight[u] for u in range(2)], axis=0)
        gain = jnp.concatenate(
            [jnp.sum(pert[u] * pull[u], axis=1, keepdims=True) for u in range(2)], axis=0
        )
        system = product(halves(scaled), halves(jnp.concatenate(pert, axis=0)), turned=True)
        return jnp.concatenate(x, axis=0).T, gain, system * same + (members - 1.0) * eye

    def second(state):
        x_turned, gain, system = state
        square = jnp.sum(system * system, axis=0, keepdims=True)
        halved = [
            jnp.sum(jnp.where(side, square, 0.0), axis=1, keepdims=True) for side in (left, ~left)
        ]
        scale_inv = lax.rsqrt(jnp.where(left, halved[0], halved[1]))
        a = system * scale_inv
        parts = halves(a)
        return x_turned, gain, scale_inv, a, product(parts, parts)

    def third(state):
        x_turned, gain, scale_inv, a, b = state
        inverse = n0 * eye + n1 * a + n2 * b + product(halves(b), halves(n3 * a + n4 * b))
        return x_turned, gain, scale_inv, inverse

    def fourth(state):
        x_turned, gain, scale_inv, inverse = state
        half_vec = jnp.sum(inverse * gain, axis=0, keepdims=True)
        centre = jnp.sum(inverse * half_vec, axis=1, keepdims=True)
        weights = inverse * jnp.sqrt((members - 1.0) * scale_inv) + centre * (same * scale_inv)
        rest = (1.0 - jnp.sum(weights, axis=0, keepdims=True)) * (1.0 / members)
        return product(halves(x_turned), halves(weights + rest * same))

    def step(g, carry):
        cell = [g * (2 * GROUP) + 2 * u for u in range(GROUP)]
        states = [first(c) for c in cell]
        states = [second(s) for s in states]
        states = [third(s) for s in states]
        results = [fourth(s) for s in states]
        for c, result in zip(cell, results):
            out[pl.ds(c, entries, stride=cells), :] = result[:, :members]
            out[pl.ds(c + 1, entries, stride=cells), :] = result[:, members:]
        return carry

    lax.fori_loop(0, cells // (2 * GROUP), step, 0)


def analyse(block, total, pulled):
    cells, entries = total.shape
    members = block.shape[0] // cells
    return pl.pallas_call(
        analyse_kernel,
        out_shape=jax.ShapeDtypeStruct((entries * cells, members), jnp.float32),
        compiler_params=GRANT,
        name="analyse",
    )(block, total, pulled)


def moved_by(value, down, right):
    rows, cols = (lax.axis_size("row"), lax.axis_size("col"))
    pairs = [
        (i * cols + j, (i + down) * cols + j + right)
        for i in range(rows)
        for j in range(cols)
        if 0 <= i + down < rows and 0 <= j + right < cols
    ]
    return lax.ppermute(value, ("row", "col"), pairs)


def body(
    background_sample,
    coupling,
    diffusion,
    wind_row,
    wind_col,
    observed_entry_index,
    obs_value,
    obs_weight,
):
    members_here, variables, levels, rows, cols = background_sample.shape
    entries = variables * levels
    dests = lax.axis_size("mem")
    top, bottom, own_w, own_e, own_nw, own_ne, own_sw, own_se = turn(background_sample)
    halos = (
        moved_by(bottom, 1, 0),
        moved_by(top, -1, 0),
        moved_by(own_e, 0, 1),
        moved_by(own_w, 0, -1),
        moved_by(own_se, 1, 1),
        moved_by(own_sw, 1, -1),
        moved_by(own_ne, -1, 1),
        moved_by(own_nw, -1, -1),
    )
    rates = jnp.concatenate(
        [
            jnp.stack([diffusion, wind_row, wind_col]),
            jnp.pad(coupling, ((0, 0), (0, levels - variables))),
        ]
    )
    sent = forecast(dests, rates, top, bottom, *halos)
    moved = lax.all_to_all(sent, "mem", split_axis=0, concat_axis=0, tiled=True)
    cells = rows * cols // dests
    members = dests * members_here

    def listed(x):
        return jnp.transpose(x, (1, 2, 0)).reshape(cells, x.shape[0])

    total, pulled = weigh(
        listed(observed_entry_index), listed(obs_value), listed(obs_weight), entries
    )
    result = analyse(moved.reshape(members * cells, entries), total, pulled)
    result = result.reshape(variables, levels, rows, cols // dests, members)
    return jnp.transpose(result, (4, 0, 1, 2, 3))


def solution(mesh):
    obs = P(None, "row", ("col", "mem"))
    return jax.shard_map(
        body,
        mesh=mesh,
        in_specs=(P("mem", None, None, "row", "col"), P(), P(), P(), P(), obs, obs, obs),
        out_specs=P(None, None, None, "row", ("col", "mem")),
        check_vma=False,
    )
```

```python
import jax
import jax.numpy as jnp
from jax import lax
from jax.experimental import pallas as pl
from jax.experimental.pallas import tpu as pltpu
from jax.sharding import PartitionSpec as P

HALO = 4
EDGE = 16
DEPTH = (14, 12, 10, 8)
GROUP = 4
GRANT = pltpu.CompilerParams(vmem_limit_bytes=14 * 2**20)
NEWTON = (2.25, -2.4375, 1.6875, -0.5625, 0.0625)


def turn_kernel(block, top, bottom, west, east):
    members, entries, rows, cols = block.shape
    flat = block.reshape(members, entries * rows, cols)
    for m in range(members):
        for i in range(rows):
            plane = flat[m, pl.ds(i, entries, stride=rows), :].T
            half = top if i < HALO else bottom
            half[m, i % HALO, HALO : HALO + cols] = plane
            west[m, i] = plane[:HALO]
            east[m, i] = plane[cols - HALO :]


def turn(block):
    members, variables, levels, rows, cols = block.shape
    entries = variables * levels
    half = jax.ShapeDtypeStruct((members, HALO, cols + 2 * HALO, entries), jnp.float32)
    side = jax.ShapeDtypeStruct((members, rows, HALO, entries), jnp.float32)
    return pl.pallas_call(
        turn_kernel,
        out_shape=[half, half, side, side],
        compiler_params=GRANT,
        name="turn",
    )(block.reshape(members, entries, rows, cols))


def widen_kernel(west, east, top_in, bottom_in, top, bottom):
    members, rows, _, _ = west.shape
    last = top.shape[2] - HALO
    for m in range(members):
        for i in range(rows):
            half = top if i < HALO else bottom
            half[m, i % HALO, :HALO] = west[m, i]
            half[m, i % HALO, last:] = east[m, i]


def widen(west, east, top, bottom):
    half = jax.ShapeDtypeStruct(top.shape, top.dtype)
    return pl.pallas_call(
        widen_kernel,
        out_shape=[half, half],
        input_output_aliases={2: 0, 3: 1},
        compiler_params=GRANT,
        name="widen",
    )(west, east, top, bottom)


def forecast_kernel(
    rates, top, bottom, north, south, out, state, slope, mixer
):
    members, _, padded, entries = top.shape
    cols = padded - 2 * HALO
    dests, listed, _ = out.shape
    cells = listed // members
    levels = rates.shape[1]
    variables = entries // levels
    share = cols // dests
    rows = 2 * HALO
    last = EDGE + cols
    inside = [
        jnp.where(test, 1.0, 0.0)
        for test in (
            lax.axis_index("row") > 0,
            lax.axis_index("row") < lax.axis_size("row") - 1,
            lax.axis_index("col") > 0,
            lax.axis_index("col") < lax.axis_size("col") - 1,
        )
    ]
    diffusion, wind_row, wind_col = (
        jnp.concatenate([rates[k : k + 1]] * variables, axis=1) for k in range(3)
    )
    c_n, c_s = (diffusion + 0.5 * wind_row, diffusion - 0.5 * wind_row)
    c_w, c_e = (diffusion + 0.5 * wind_col, diffusion - 0.5 * wind_col)
    source = lax.broadcasted_iota(jnp.int32, (entries, entries), 0)
    target = lax.broadcasted_iota(jnp.int32, (entries, entries), 1)
    mixing = jnp.where(source == target, -4.0 * diffusion, 0.0)
    for v in range(variables):
        for w in range(variables):
            hit = (target - source == levels * (v - w)) & (target // levels == v)
            mixing += jnp.where(hit, rates[3 + v : 4 + v, w : w + 1], 0.0)
    mixer[...] = jnp.concatenate([jnp.concatenate(halves(mixing), axis=1)] * 2, axis=0)

    def tendency(field, i, deep, start, size):
        here = field[pl.ds(i, deep), pl.ds(start, size), :]
        parts = jnp.concatenate(halves(here), axis=2).reshape(deep * size, 2 * entries)
        both = lax.dot_general(
            parts, mixer[...], (((1,), (0,)), ((), ())), preferred_element_type=jnp.float32
        )
        total = c_n * field[pl.ds(i - 1, deep), pl.ds(start, size), :]
        total += c_s * field[pl.ds(i + 1, deep), pl.ds(start, size), :]
        total += c_w * field[pl.ds(i, deep), pl.ds(start - 1, size), :]
        total += c_e * field[pl.ds(i, deep), pl.ds(start + 1, size), :]
        both = both.reshape(deep, size, 2 * entries)
        return here, total + (both[:, :, :entries] + both[:, :, entries:])

    def masked(value, i):
        deep, size, _ = value.shape
        row = i + lax.broadcasted_iota(jnp.int32, (deep, 1, 1), 0)
        value = value * jnp.where(row < HALO, inside[0], jnp.where(row >= 3 * HALO, inside[1], 1.0))
        where = first + lax.broadcasted_iota(jnp.int32, (1, size, 1), 1)
        return value * jnp.where(where < EDGE, inside[2], jnp.where(where >= last, inside[3], 1.0))

    first, wide = (EDGE - 8, cols + 16)

    def rates_of(low, high, deep):
        def step(b, carry):
            i = low + deep * b
            here, total = tendency(state, i, deep, first, wide)
            slope[pl.ds(i, deep), pl.ds(first, wide), :] = masked(total, i)
            return carry

        lax.fori_loop(0, (high - low) // deep, step, 0)

    def update(low, high, deep):
        def step(b, carry):
            i = low + deep * b
            here, total = tendency(slope, i, deep, first, wide)
            new = state[pl.ds(i, deep), pl.ds(first, wide), :] + here + 0.5 * total
            state[pl.ds(i, deep), pl.ds(first, wide), :] = masked(new, i)
            return carry

        lax.fori_loop(0, (high - low) // deep, step, 0)

    def member(m, carry):
        for i in range(HALO):
            for at, rows_here in enumerate((north, top, bottom, south)):
                state[HALO * at + i, EDGE - HALO : last + HALO] = rows_here[m, i]
        rates_of(1, 15, DEPTH[0])
        update(2, 14, DEPTH[1])
        rates_of(3, 13, DEPTH[2])
        for i in range(0, rows, DEPTH[3]):
            here, total = tendency(slope, HALO + i, DEPTH[3], EDGE, cols)
            new = state[HALO + i : HALO + i + DEPTH[3], EDGE:last] + here + 0.5 * total
            for r in range(DEPTH[3]):
                for d in range(dests):
                    out[d, pl.ds(m * cells + (i + r) * share, share), :] = new[r, d * share : (d + 1) * share]
        return carry

    lax.fori_loop(0, members, member, 0)


def forecast(dests, *operands):
    members, _, padded, entries = operands[1].shape
    cols = padded - 2 * HALO
    cells = 2 * HALO * cols // dests
    return pl.pallas_call(
        forecast_kernel,
        out_shape=jax.ShapeDtypeStruct((dests, members * cells, entries), jnp.float32),
        scratch_shapes=[pltpu.VMEM((4 * HALO, cols + 2 * EDGE, entries), jnp.float32)] * 2
        + [pltpu.VMEM((2 * entries, 2 * entries), jnp.bfloat16)],
        compiler_params=GRANT,
        name="forecast",
    )(*operands)


def weigh_kernel(index, value, weight, total, pulled):
    cells, observations = index.shape
    entries = total.shape[1]
    entry = lax.broadcasted_iota(jnp.int32, (cells, entries), 1)
    w = weight[...]
    wv = w * value[...]
    acc = jnp.zeros((cells, entries), jnp.float32)
    acc_v = jnp.zeros((cells, entries), jnp.float32)
    named = index[...]
    for k in range(observations):
        hit = jnp.broadcast_to(named[:, k : k + 1], (cells, entries)) == entry
        acc += jnp.where(hit, jnp.broadcast_to(w[:, k : k + 1], (cells, entries)), 0.0)
        acc_v += jnp.where(hit, jnp.broadcast_to(wv[:, k : k + 1], (cells, entries)), 0.0)
    total[...] = acc
    pulled[...] = acc_v


def weigh(index, value, weight, entries):
    shape = jax.ShapeDtypeStruct((index.shape[0], entries), jnp.float32)
    return pl.pallas_call(weigh_kernel, out_shape=[shape, shape], compiler_params=GRANT, name="weigh")(
        index, value, weight
    )


def halves(value):
    high = value.astype(jnp.bfloat16)
    return high, (value - high.astype(jnp.float32)).astype(jnp.bfloat16)


def product(a, b, turned=False):
    (ah, al), (bh, bl) = (a, b)
    dot = lambda u, v: lax.dot_general(
        u, v, (((1,), (1 if turned else 0,)), ((), ())), preferred_element_type=jnp.float32
    )
    both = dot(jnp.concatenate([ah, ah], axis=1), jnp.concatenate([bh, bl], axis=1 if turned else 0))
    return both + dot(al, bh)


def analyse_kernel(block, total, pulled, out):
    cells = total.shape[0]
    members = block.shape[0] // cells
    entries = block.shape[1]
    pair = 2 * members
    row_id = lax.broadcasted_iota(jnp.int32, (pair, pair), 0)
    col_id = lax.broadcasted_iota(jnp.int32, (pair, pair), 1)
    eye = (row_id == col_id).astype(jnp.float32)
    same = ((row_id < members) == (col_id < members)).astype(jnp.float32)
    left = lax.broadcasted_iota(jnp.int32, (1, pair), 1) < members
    n0, n1, n2, n3, n4 = NEWTON
    spread = lambda row: jnp.broadcast_to(row, (members, entries))

    def first(cell):
        x = [block[pl.ds(cell + u, members, stride=cells), :] for u in range(2)]
        mean = [jnp.sum(v, axis=0, keepdims=True) * (1.0 / members) for v in x]
        weight = [total[pl.ds(cell + u, 1), :] for u in range(2)]
        pull = [pulled[pl.ds(cell + u, 1), :] - mean[u] * weight[u] for u in range(2)]
        pert = [x[u] - mean[u] for u in range(2)]
        scaled = jnp.concatenate([pert[u] * weight[u] for u in range(2)], axis=0)
        gain = jnp.concatenate(
            [jnp.sum(pert[u] * pull[u], axis=1, keepdims=True) for u in range(2)], axis=0
        )
        system = product(halves(scaled), halves(jnp.concatenate(pert, axis=0)), turned=True)
        return jnp.concatenate(x, axis=0).T, gain, system * same + (members - 1.0) * eye

    def second(state):
        x_turned, gain, system = state
        square = jnp.sum(system * system, axis=0, keepdims=True)
        halved = [
            jnp.sum(jnp.where(side, square, 0.0), axis=1, keepdims=True) for side in (left, ~left)
        ]
        scale_inv = lax.rsqrt(jnp.where(left, halved[0], halved[1]))
        a = system * scale_inv
        parts = halves(a)
        return x_turned, gain, scale_inv, a, product(parts, parts)

    def third(state):
        x_turned, gain, scale_inv, a, b = state
        inverse = n0 * eye + n1 * a + n2 * b + product(halves(b), halves(n3 * a + n4 * b))
        return x_turned, gain, scale_inv, inverse

    def fourth(state):
        x_turned, gain, scale_inv, inverse = state
        half_vec = jnp.sum(inverse * gain, axis=0, keepdims=True)
        centre = jnp.sum(inverse * half_vec, axis=1, keepdims=True)
        weights = inverse * jnp.sqrt((members - 1.0) * scale_inv) + centre * (same * scale_inv)
        rest = (1.0 - jnp.sum(weights, axis=0, keepdims=True)) * (1.0 / members)
        return product(halves(x_turned), halves(weights + rest * same))

    def step(g, carry):
        cell = [g * (2 * GROUP) + 2 * u for u in range(GROUP)]
        states = [first(c) for c in cell]
        states = [second(s) for s in states]
        states = [third(s) for s in states]
        results = [fourth(s) for s in states]
        for c, result in zip(cell, results):
            out[pl.ds(c, entries, stride=cells), :] = result[:, :members]
            out[pl.ds(c + 1, entries, stride=cells), :] = result[:, members:]
        return carry

    lax.fori_loop(0, cells // (2 * GROUP), step, 0)


def analyse(block, total, pulled):
    cells, entries = total.shape
    members = block.shape[0] // cells
    return pl.pallas_call(
        analyse_kernel,
        out_shape=jax.ShapeDtypeStruct((entries * cells, members), jnp.float32),
        compiler_params=GRANT,
        name="analyse",
    )(block, total, pulled)


def moved_by(value, down, right):
    rows, cols = (lax.axis_size("row"), lax.axis_size("col"))
    pairs = [
        (i * cols + j, (i + down) * cols + j + right)
        for i in range(rows)
        for j in range(cols)
        if 0 <= i + down < rows and 0 <= j + right < cols
    ]
    return lax.ppermute(value, ("row", "col"), pairs)


def body(
    background_sample,
    coupling,
    diffusion,
    wind_row,
    wind_col,
    observed_entry_index,
    obs_value,
    obs_weight,
):
    members_here, variables, levels, rows, cols = background_sample.shape
    entries = variables * levels
    dests = lax.axis_size("mem")
    top, bottom, own_w, own_e = turn(background_sample)
    top, bottom = widen(moved_by(own_e, 0, 1), moved_by(own_w, 0, -1), top, bottom)
    north, south = (moved_by(bottom, 1, 0), moved_by(top, -1, 0))
    rates = jnp.concatenate(
        [
            jnp.stack([diffusion, wind_row, wind_col]),
            jnp.pad(coupling, ((0, 0), (0, levels - variables))),
        ]
    )
    sent = forecast(dests, rates, top, bottom, north, south)
    moved = lax.all_to_all(sent, "mem", split_axis=0, concat_axis=0, tiled=True)
    cells = rows * cols // dests
    members = dests * members_here

    def listed(x):
        return jnp.transpose(x, (1, 2, 0)).reshape(cells, x.shape[0])

    total, pulled = weigh(
        listed(observed_entry_index), listed(obs_value), listed(obs_weight), entries
    )
    result = analyse(moved.reshape(members * cells, entries), total, pulled)
    result = result.reshape(variables, levels, rows, cols // dests, members)
    return jnp.transpose(result, (4, 0, 1, 2, 3))


def solution(mesh):
    obs = P(None, "row", ("col", "mem"))
    return jax.shard_map(
        body,
        mesh=mesh,
        in_specs=(P("mem", None, None, "row", "col"), P(), P(), P(), P(), obs, obs, obs),
        out_specs=P(None, None, None, "row", ("col", "mem")),
        check_vma=False,
    )
```

```python
import jax
import jax.numpy as jnp
from jax import lax
from jax.experimental import pallas as pl
from jax.experimental.pallas import tpu as pltpu
from jax.sharding import PartitionSpec as P

HALO = 4
EDGE = 16
DEPTH = (14, 12, 10, 8)
GROUP = 8
IN_STEP = 33
OUT_STEP = 40
GRANT = pltpu.CompilerParams(vmem_limit_bytes=14 * 2**20)
NEWTON = (2.25, -2.4375, 1.6875, -0.5625, 0.0625)


def turn_kernel(block, top, bottom, west, east):
    members, entries, rows, cols = block.shape
    flat = block.reshape(members, entries * rows, cols)
    for m in range(members):
        for i in range(rows):
            plane = flat[m, pl.ds(i, entries, stride=rows), :].T
            half = top if i < HALO else bottom
            half[m, i % HALO] = plane
            west[m, i] = plane[:HALO]
            east[m, i] = plane[cols - HALO :]


def turn(block):
    members, variables, levels, rows, cols = block.shape
    entries = variables * levels
    half = jax.ShapeDtypeStruct((members, HALO, cols, entries), jnp.float32)
    side = jax.ShapeDtypeStruct((members, rows, HALO, entries), jnp.float32)
    return pl.pallas_call(
        turn_kernel,
        out_shape=[half, half, side, side],
        compiler_params=GRANT,
        name="turn",
    )(block.reshape(members, entries, rows, cols))


def forecast_kernel(
    rates, top, bottom, north, south, west, east, corner_n, corner_s, out, state, slope, mixer
):
    members, _, cols, entries = top.shape
    dests, listed, _ = out.shape
    cells = listed // members
    levels = rates.shape[1]
    variables = entries // levels
    share = cols // dests
    rows = 2 * HALO
    last = EDGE + cols
    inside = [
        jnp.where(test, 1.0, 0.0)
        for test in (
            lax.axis_index("row") > 0,
            lax.axis_index("row") < lax.axis_size("row") - 1,
            lax.axis_index("col") > 0,
            lax.axis_index("col") < lax.axis_size("col") - 1,
        )
    ]
    diffusion, wind_row, wind_col = (
        jnp.concatenate([rates[k : k + 1]] * variables, axis=1) for k in range(3)
    )
    c_n, c_s = (diffusion + 0.5 * wind_row, diffusion - 0.5 * wind_row)
    c_w, c_e = (diffusion + 0.5 * wind_col, diffusion - 0.5 * wind_col)
    source = lax.broadcasted_iota(jnp.int32, (entries, entries), 0)
    target = lax.broadcasted_iota(jnp.int32, (entries, entries), 1)
    mixing = jnp.where(source == target, -4.0 * diffusion, 0.0)
    for v in range(variables):
        for w in range(variables):
            hit = (target - source == levels * (v - w)) & (target // levels == v)
            mixing += jnp.where(hit, rates[3 + v : 4 + v, w : w + 1], 0.0)
    mixer[...] = jnp.concatenate([jnp.concatenate(halves(mixing), axis=1)] * 2, axis=0)

    def tendency(field, i, deep, start, size):
        here = field[pl.ds(i, deep), pl.ds(start, size), :]
        parts = jnp.concatenate(halves(here), axis=2).reshape(deep * size, 2 * entries)
        both = lax.dot_general(
            parts, mixer[...], (((1,), (0,)), ((), ())), preferred_element_type=jnp.float32
        )
        total = c_n * field[pl.ds(i - 1, deep), pl.ds(start, size), :]
        total += c_s * field[pl.ds(i + 1, deep), pl.ds(start, size), :]
        total += c_w * field[pl.ds(i, deep), pl.ds(start - 1, size), :]
        total += c_e * field[pl.ds(i, deep), pl.ds(start + 1, size), :]
        both = both.reshape(deep, size, 2 * entries)
        return here, total + (both[:, :, :entries] + both[:, :, entries:])

    def masked(value, i):
        deep, size, _ = value.shape
        row = i + lax.broadcasted_iota(jnp.int32, (deep, 1, 1), 0)
        value = value * jnp.where(row < HALO, inside[0], jnp.where(row >= 3 * HALO, inside[1], 1.0))
        where = first + lax.broadcasted_iota(jnp.int32, (1, size, 1), 1)
        return value * jnp.where(where < EDGE, inside[2], jnp.where(where >= last, inside[3], 1.0))

    first, wide = (EDGE - 8, cols + 16)

    def rates_of(low, high, deep):
        def step(b, carry):
            i = low + deep * b
            here, total = tendency(state, i, deep, first, wide)
            slope[pl.ds(i, deep), pl.ds(first, wide), :] = masked(total, i)
            return carry

        lax.fori_loop(0, (high - low) // deep, step, 0)

    def update(low, high, deep):
        def step(b, carry):
            i = low + deep * b
            here, total = tendency(slope, i, deep, first, wide)
            new = state[pl.ds(i, deep), pl.ds(first, wide), :] + here + 0.5 * total
            state[pl.ds(i, deep), pl.ds(first, wide), :] = masked(new, i)
            return carry

        lax.fori_loop(0, (high - low) // deep, step, 0)

    def member(m, carry):
        for i in range(HALO):
            state[i, EDGE:last] = north[m, i]
            state[HALO + i, EDGE:last] = top[m, i]
            state[2 * HALO + i, EDGE:last] = bottom[m, i]
            state[3 * HALO + i, EDGE:last] = south[m, i]
            state[i, EDGE - HALO : EDGE] = corner_n[m, i, :HALO]
            state[i, last : last + HALO] = corner_n[m, i, HALO:]
            state[3 * HALO + i, EDGE - HALO : EDGE] = corner_s[m, i, :HALO]
            state[3 * HALO + i, last : last + HALO] = corner_s[m, i, HALO:]
        for i in range(rows):
            state[HALO + i, EDGE - HALO : EDGE] = west[m, i]
            state[HALO + i, last : last + HALO] = east[m, i]
        rates_of(1, 15, DEPTH[0])
        update(2, 14, DEPTH[1])
        rates_of(3, 13, DEPTH[2])
        for i in range(0, rows, DEPTH[3]):
            here, total = tendency(slope, HALO + i, DEPTH[3], EDGE, cols)
            new = state[HALO + i : HALO + i + DEPTH[3], EDGE:last] + here + 0.5 * total
            for r in range(DEPTH[3]):
                for d in range(dests):
                    out[d, pl.ds(m * cells + (i + r) * share, share), :] = new[r, d * share : (d + 1) * share]
        return carry

    lax.fori_loop(0, members, member, 0)


def forecast(rates, top, bottom, north, south, west, east, corner_n, corner_s, dests):
    members, _, cols, entries = top.shape
    cells = 2 * HALO * cols // dests
    return pl.pallas_call(
        forecast_kernel,
        out_shape=jax.ShapeDtypeStruct((dests, members * cells, entries), jnp.float32),
        scratch_shapes=[pltpu.VMEM((4 * HALO, cols + 2 * EDGE, entries), jnp.float32)] * 2
        + [pltpu.VMEM((2 * entries, 2 * entries), jnp.bfloat16)],
        compiler_params=GRANT,
        name="forecast",
    )(rates, top, bottom, north, south, west, east, corner_n, corner_s)


def weigh_kernel(index, value, weight, total, pulled):
    cells, observations = index.shape
    entries = total.shape[1]
    entry = lax.broadcasted_iota(jnp.int32, (cells, entries), 1)
    w = weight[...]
    wv = w * value[...]
    acc = jnp.zeros((cells, entries), jnp.float32)
    acc_v = jnp.zeros((cells, entries), jnp.float32)
    named = index[...]
    for k in range(observations):
        hit = jnp.broadcast_to(named[:, k : k + 1], (cells, entries)) == entry
        acc += jnp.where(hit, jnp.broadcast_to(w[:, k : k + 1], (cells, entries)), 0.0)
        acc_v += jnp.where(hit, jnp.broadcast_to(wv[:, k : k + 1], (cells, entries)), 0.0)
    total[...] = acc
    pulled[...] = acc_v


def weigh(index, value, weight, entries):
    shape = jax.ShapeDtypeStruct((index.shape[0], entries), jnp.float32)
    return pl.pallas_call(weigh_kernel, out_shape=[shape, shape], compiler_params=GRANT, name="weigh")(
        index, value, weight
    )


def halves(value):
    high = value.astype(jnp.bfloat16)
    return high, (value - high.astype(jnp.float32)).astype(jnp.bfloat16)


def product(a, b, turned=False):
    (ah, al), (bh, bl) = (a, b)
    dot = lambda u, v: lax.dot_general(
        u, v, (((1,), (1 if turned else 0,)), ((), ())), preferred_element_type=jnp.float32
    )
    both = dot(jnp.concatenate([ah, ah], axis=1), jnp.concatenate([bh, bl], axis=1 if turned else 0))
    return both + dot(al, bh)


def analyse_kernel(block, total, pulled, out, spaced, results, sems):
    cells = total.shape[0]
    members = block.shape[0] // cells
    entries = block.shape[1]
    pair = 2 * members
    for n in range(members):
        spaced[n * IN_STEP : n * IN_STEP + cells, :] = block[n * cells : (n + 1) * cells, :]
    row_id = lax.broadcasted_iota(jnp.int32, (pair, pair), 0)
    col_id = lax.broadcasted_iota(jnp.int32, (pair, pair), 1)
    eye = (row_id == col_id).astype(jnp.float32)
    same = ((row_id < members) == (col_id < members)).astype(jnp.float32)
    left = lax.broadcasted_iota(jnp.int32, (1, pair), 1) < members
    n0, n1, n2, n3, n4 = NEWTON
    spread = lambda row: jnp.broadcast_to(row, (members, entries))

    def first(cell):
        x = [spaced[pl.ds(cell + u, members, stride=IN_STEP), :] for u in range(2)]
        mean = [jnp.sum(v, axis=0, keepdims=True) * (1.0 / members) for v in x]
        weight = [total[pl.ds(cell + u, 1), :] for u in range(2)]
        pull = [pulled[pl.ds(cell + u, 1), :] - mean[u] * weight[u] for u in range(2)]
        pert = [x[u] - mean[u] for u in range(2)]
        scaled = jnp.concatenate([pert[u] * weight[u] for u in range(2)], axis=0)
        gain = jnp.concatenate(
            [jnp.sum(pert[u] * pull[u], axis=1, keepdims=True) for u in range(2)], axis=0
        )
        system = product(halves(scaled), halves(jnp.concatenate(pert, axis=0)), turned=True)
        return jnp.concatenate(x, axis=0).T, gain, system * same + (members - 1.0) * eye

    def second(state):
        x_turned, gain, system = state
        square = jnp.sum(system * system, axis=0, keepdims=True)
        halved = [
            jnp.sum(jnp.where(side, square, 0.0), axis=1, keepdims=True) for side in (left, ~left)
        ]
        scale_inv = lax.rsqrt(jnp.where(left, halved[0], halved[1]))
        a = system * scale_inv
        parts = halves(a)
        return x_turned, gain, scale_inv, a, product(parts, parts)

    def third(state):
        x_turned, gain, scale_inv, a, b = state
        inverse = n0 * eye + n1 * a + n2 * b + product(halves(b), halves(n3 * a + n4 * b))
        return x_turned, gain, scale_inv, inverse

    def fourth(state):
        x_turned, gain, scale_inv, inverse = state
        half_vec = jnp.sum(inverse * gain, axis=0, keepdims=True)
        centre = jnp.sum(inverse * half_vec, axis=1, keepdims=True)
        weights = inverse * jnp.sqrt((members - 1.0) * scale_inv) + centre * (same * scale_inv)
        rest = (1.0 - jnp.sum(weights, axis=0, keepdims=True)) * (1.0 / members)
        return product(halves(x_turned), halves(weights + rest * same))

    copies = []
    span = 2 * GROUP
    for g in range(cells // span):
        cell = [g * span + 2 * u for u in range(GROUP)]
        states = [first(c) for c in cell]
        states = [second(s) for s in states]
        states = [third(s) for s in states]
        finished = [fourth(s) for s in states]
        for c, result in zip(cell, finished):
            results[pl.ds(c, entries, stride=OUT_STEP), :] = result[:, :members]
            results[pl.ds(c + 1, entries, stride=OUT_STEP), :] = result[:, members:]
        here = pl.ds(g * span, span)
        source = results.reshape(entries, OUT_STEP, members).at[:, here, :]
        copies.append(pltpu.make_async_copy(source, out.at[:, here, :], sems.at[g]))
        copies[-1].start()
    for copy in copies:
        copy.wait()


def analyse(block, total, pulled):
    cells, entries = total.shape
    members = block.shape[0] // cells
    return pl.pallas_call(
        analyse_kernel,
        out_shape=jax.ShapeDtypeStruct((entries, cells, members), jnp.float32),
        out_specs=pl.BlockSpec(memory_space=pl.ANY),
        scratch_shapes=[
            pltpu.VMEM((members * IN_STEP, entries), jnp.float32),
            pltpu.VMEM((entries * OUT_STEP, members), jnp.float32),
            pltpu.SemaphoreType.DMA((cells // (2 * GROUP),)),
        ],
        compiler_params=GRANT,
        name="analyse",
    )(block, total, pulled)


def neighbours(axis):
    up = [(i, i + 1) for i in range(lax.axis_size(axis) - 1)]
    return up, [(j, i) for i, j in up]


def body(
    background_sample,
    coupling,
    diffusion,
    wind_row,
    wind_col,
    observed_entry_index,
    obs_value,
    obs_weight,
):
    members_here, variables, levels, rows, cols = background_sample.shape
    entries = variables * levels
    dests = lax.axis_size("mem")
    top, bottom, own_w, own_e = turn(background_sample)
    col_up, col_down = neighbours("col")
    row_up, row_down = neighbours("row")
    west = lax.ppermute(own_e, "col", col_up)
    east = lax.ppermute(own_w, "col", col_down)
    north = lax.ppermute(bottom, "row", row_up)
    south = lax.ppermute(top, "row", row_down)
    sides = jnp.concatenate([west, east], axis=2)
    corner_n = lax.ppermute(sides[:, HALO:], "row", row_up)
    corner_s = lax.ppermute(sides[:, :HALO], "row", row_down)

    rates = jnp.concatenate(
        [
            jnp.stack([diffusion, wind_row, wind_col]),
            jnp.pad(coupling, ((0, 0), (0, levels - variables))),
        ]
    )
    sent = forecast(
        rates, top, bottom, north, south, west, east, corner_n, corner_s, dests
    )
    moved = lax.all_to_all(sent, "mem", split_axis=0, concat_axis=0, tiled=True)
    cells = rows * cols // dests
    members = dests * members_here

    def listed(x):
        return jnp.transpose(x, (1, 2, 0)).reshape(cells, x.shape[0])

    total, pulled = weigh(
        listed(observed_entry_index), listed(obs_value), listed(obs_weight), entries
    )
    result = analyse(moved.reshape(members * cells, entries), total, pulled)
    result = result.reshape(variables, levels, rows, cols // dests, members)
    return jnp.transpose(result, (4, 0, 1, 2, 3))


def solution(mesh):
    obs = P(None, "row", ("col", "mem"))
    return jax.shard_map(
        body,
        mesh=mesh,
        in_specs=(P("mem", None, None, "row", "col"), P(), P(), P(), P(), obs, obs, obs),
        out_specs=P(None, None, None, "row", ("col", "mem")),
        check_vma=False,
    )
```

```python
import functools

import jax
import jax.numpy as jnp
from jax import lax
from jax.experimental import pallas as pl
from jax.experimental.pallas import tpu as pltpu
from jax.sharding import PartitionSpec as P


HALO = 4
EDGE = 16
DEPTH = (14, 12, 10, 8)
GROUP = 8
IN_STEP = 33
OUT_STEP = 40
GRANT = pltpu.CompilerParams(vmem_limit_bytes=14 * 2**20)
NEWTON = (2.25, -2.4375, 1.6875, -0.5625, 0.0625)


def turn_kernel(block, west, east, *halves_out):
    members, entries, rows, cols = block.shape
    flat = block.reshape(members, entries * rows, cols)
    for m in range(members):
        for i in range(rows):
            plane = flat[m, pl.ds(i, entries, stride=rows), :].T
            halves_out[2 * m + i // HALO][i % HALO] = plane
            west[m, i] = plane[:HALO]
            east[m, i] = plane[cols - HALO :]


def turn(block):
    members, variables, levels, rows, cols = block.shape
    entries = variables * levels
    half = jax.ShapeDtypeStruct((HALO, cols, entries), jnp.float32)
    side = jax.ShapeDtypeStruct((members, rows, HALO, entries), jnp.float32)
    return pl.pallas_call(
        turn_kernel,
        out_shape=[side, side] + [half] * (2 * members),
        compiler_params=GRANT,
        name="turn",
    )(block.reshape(members, entries, rows, cols))


def forecast_kernel(
    m, rates, top, bottom, north, south, west, east, corner_n, corner_s, out, state, slope, mixer
):
    _, cols, entries = top.shape
    dests = out.shape[0]
    levels = rates.shape[1]
    variables = entries // levels
    share = cols // dests
    rows = 2 * HALO
    last = EDGE + cols
    inside = [
        jnp.where(test, 1.0, 0.0)
        for test in (
            lax.axis_index("row") > 0,
            lax.axis_index("row") < lax.axis_size("row") - 1,
            lax.axis_index("col") > 0,
            lax.axis_index("col") < lax.axis_size("col") - 1,
        )
    ]
    diffusion, wind_row, wind_col = (
        jnp.concatenate([rates[k : k + 1]] * variables, axis=1) for k in range(3)
    )
    c_n, c_s = (diffusion + 0.5 * wind_row, diffusion - 0.5 * wind_row)
    c_w, c_e = (diffusion + 0.5 * wind_col, diffusion - 0.5 * wind_col)
    source = lax.broadcasted_iota(jnp.int32, (entries, entries), 0)
    target = lax.broadcasted_iota(jnp.int32, (entries, entries), 1)
    mixing = jnp.where(source == target, -4.0 * diffusion, 0.0)
    for v in range(variables):
        for w in range(variables):
            hit = (target - source == levels * (v - w)) & (target // levels == v)
            mixing += jnp.where(hit, rates[3 + v : 4 + v, w : w + 1], 0.0)
    mixer[...] = jnp.concatenate([jnp.concatenate(halves(mixing), axis=1)] * 2, axis=0)

    def tendency(field, i, deep, start, size):
        here = field[pl.ds(i, deep), pl.ds(start, size), :]
        parts = jnp.concatenate(halves(here), axis=2).reshape(deep * size, 2 * entries)
        both = lax.dot_general(
            parts, mixer[...], (((1,), (0,)), ((), ())), preferred_element_type=jnp.float32
        )
        total = c_n * field[pl.ds(i - 1, deep), pl.ds(start, size), :]
        total += c_s * field[pl.ds(i + 1, deep), pl.ds(start, size), :]
        total += c_w * field[pl.ds(i, deep), pl.ds(start - 1, size), :]
        total += c_e * field[pl.ds(i, deep), pl.ds(start + 1, size), :]
        both = both.reshape(deep, size, 2 * entries)
        return here, total + (both[:, :, :entries] + both[:, :, entries:])

    def masked(value, i):
        deep, size, _ = value.shape
        row = i + lax.broadcasted_iota(jnp.int32, (deep, 1, 1), 0)
        value = value * jnp.where(row < HALO, inside[0], jnp.where(row >= 3 * HALO, inside[1], 1.0))
        where = first + lax.broadcasted_iota(jnp.int32, (1, size, 1), 1)
        return value * jnp.where(where < EDGE, inside[2], jnp.where(where >= last, inside[3], 1.0))

    first, wide = (EDGE - 8, cols + 16)

    def rates_of(low, high, deep):
        def step(b, carry):
            i = low + deep * b
            _, total = tendency(state, i, deep, first, wide)
            slope[pl.ds(i, deep), pl.ds(first, wide), :] = masked(total, i)
            return carry

        lax.fori_loop(0, (high - low) // deep, step, 0)

    def update(low, high, deep):
        def step(b, carry):
            i = low + deep * b
            here, total = tendency(slope, i, deep, first, wide)
            new = state[pl.ds(i, deep), pl.ds(first, wide), :] + here + 0.5 * total
            state[pl.ds(i, deep), pl.ds(first, wide), :] = masked(new, i)
            return carry

        lax.fori_loop(0, (high - low) // deep, step, 0)

    for i in range(HALO):
        for at, rows_here in enumerate((north, top, bottom, south)):
            state[HALO * at + i, EDGE:last] = rows_here[i]
        state[i, EDGE - HALO : EDGE] = corner_n[m, i, :HALO]
        state[i, last : last + HALO] = corner_n[m, i, HALO:]
        state[3 * HALO + i, EDGE - HALO : EDGE] = corner_s[m, i, :HALO]
        state[3 * HALO + i, last : last + HALO] = corner_s[m, i, HALO:]
    for i in range(rows):
        state[HALO + i, EDGE - HALO : EDGE] = west[m, i]
        state[HALO + i, last : last + HALO] = east[m, i]
    rates_of(1, 15, DEPTH[0])
    update(2, 14, DEPTH[1])
    rates_of(3, 13, DEPTH[2])
    for i in range(0, rows, DEPTH[3]):
        here, total = tendency(slope, HALO + i, DEPTH[3], EDGE, cols)
        new = state[HALO + i : HALO + i + DEPTH[3], EDGE:last] + here + 0.5 * total
        for r in range(DEPTH[3]):
            for d in range(dests):
                out[d, pl.ds((i + r) * share, share), :] = new[r, d * share : (d + 1) * share]


def forecast(m, dests, *operands):
    _, cols, entries = operands[1].shape
    cells = 2 * HALO * cols // dests
    return pl.pallas_call(
        functools.partial(forecast_kernel, m),
        out_shape=jax.ShapeDtypeStruct((dests, cells, entries), jnp.float32),
        scratch_shapes=[pltpu.VMEM((4 * HALO, cols + 2 * EDGE, entries), jnp.float32)] * 2
        + [pltpu.VMEM((2 * entries, 2 * entries), jnp.bfloat16)],
        compiler_params=GRANT,
        name="forecast",
    )(*operands)


def weigh_kernel(index, value, weight, total, pulled):
    cells, observations = index.shape
    entries = total.shape[1]
    entry = lax.broadcasted_iota(jnp.int32, (cells, entries), 1)
    w = weight[...]
    wv = w * value[...]
    acc = jnp.zeros((cells, entries), jnp.float32)
    acc_v = jnp.zeros((cells, entries), jnp.float32)
    named = index[...]
    for k in range(observations):
        hit = jnp.broadcast_to(named[:, k : k + 1], (cells, entries)) == entry
        acc += jnp.where(hit, jnp.broadcast_to(w[:, k : k + 1], (cells, entries)), 0.0)
        acc_v += jnp.where(hit, jnp.broadcast_to(wv[:, k : k + 1], (cells, entries)), 0.0)
    total[...] = acc
    pulled[...] = acc_v


def weigh(index, value, weight, entries):
    shape = jax.ShapeDtypeStruct((index.shape[0], entries), jnp.float32)
    return pl.pallas_call(weigh_kernel, out_shape=[shape, shape], compiler_params=GRANT, name="weigh")(
        index, value, weight
    )


def halves(value):
    high = value.astype(jnp.bfloat16)
    return high, (value - high.astype(jnp.float32)).astype(jnp.bfloat16)


def product(a, b, turned=False):
    (ah, al), (bh, bl) = (a, b)
    dot = lambda u, v: lax.dot_general(
        u, v, (((1,), (1 if turned else 0,)), ((), ())), preferred_element_type=jnp.float32
    )
    both = dot(jnp.concatenate([ah, ah], axis=1), jnp.concatenate([bh, bl], axis=1 if turned else 0))
    return both + dot(al, bh)


def analyse_kernel(blocks, total, pulled, out, spaced, results, sems):
    cells = total.shape[0]
    parts = len(blocks)
    members = parts * blocks[0].shape[0]
    entries = total.shape[1]
    pair = 2 * members
    for n in range(members):
        spaced[n * IN_STEP : n * IN_STEP + cells, :] = blocks[n % parts][n // parts]
    row_id = lax.broadcasted_iota(jnp.int32, (pair, pair), 0)
    col_id = lax.broadcasted_iota(jnp.int32, (pair, pair), 1)
    eye = (row_id == col_id).astype(jnp.float32)
    same = ((row_id < members) == (col_id < members)).astype(jnp.float32)
    left = lax.broadcasted_iota(jnp.int32, (1, pair), 1) < members
    n0, n1, n2, n3, n4 = NEWTON

    def first(cell):
        x = [spaced[pl.ds(cell + u, members, stride=IN_STEP), :] for u in range(2)]
        mean = [jnp.sum(v, axis=0, keepdims=True) * (1.0 / members) for v in x]
        weight = [total[pl.ds(cell + u, 1), :] for u in range(2)]
        pull = [pulled[pl.ds(cell + u, 1), :] - mean[u] * weight[u] for u in range(2)]
        pert = [x[u] - mean[u] for u in range(2)]
        scaled = jnp.concatenate([pert[u] * weight[u] for u in range(2)], axis=0)
        gain = jnp.concatenate(
            [jnp.sum(pert[u] * pull[u], axis=1, keepdims=True) for u in range(2)], axis=0
        )
        system = product(halves(scaled), halves(jnp.concatenate(pert, axis=0)), turned=True)
        return jnp.concatenate(x, axis=0).T, gain, system * same + (members - 1.0) * eye

    def second(state):
        x_turned, gain, system = state
        square = jnp.sum(system * system, axis=0, keepdims=True)
        halved = [
            jnp.sum(jnp.where(side, square, 0.0), axis=1, keepdims=True) for side in (left, ~left)
        ]
        scale_inv = lax.rsqrt(jnp.where(left, halved[0], halved[1]))
        a = system * scale_inv
        parts = halves(a)
        return x_turned, gain, scale_inv, a, product(parts, parts)

    def third(state):
        x_turned, gain, scale_inv, a, b = state
        inverse = n0 * eye + n1 * a + n2 * b + product(halves(b), halves(n3 * a + n4 * b))
        return x_turned, gain, scale_inv, inverse

    def fourth(state):
        x_turned, gain, scale_inv, inverse = state
        half_vec = jnp.sum(inverse * gain, axis=0, keepdims=True)
        centre = jnp.sum(inverse * half_vec, axis=1, keepdims=True)
        weights = inverse * jnp.sqrt((members - 1.0) * scale_inv) + centre * (same * scale_inv)
        rest = (1.0 - jnp.sum(weights, axis=0, keepdims=True)) * (1.0 / members)
        return product(halves(x_turned), halves(weights + rest * same))

    copies = []
    span = 2 * GROUP
    for g in range(cells // span):
        cell = [g * span + 2 * u for u in range(GROUP)]
        states = [first(c) for c in cell]
        states = [second(s) for s in states]
        states = [third(s) for s in states]
        finished = [fourth(s) for s in states]
        for c, result in zip(cell, finished):
            results[pl.ds(c, entries, stride=OUT_STEP), :] = result[:, :members]
            results[pl.ds(c + 1, entries, stride=OUT_STEP), :] = result[:, members:]
        here = pl.ds(g * span, span)
        source = results.reshape(entries, OUT_STEP, members).at[:, here, :]
        copies.append(pltpu.make_async_copy(source, out.at[:, here, :], sems.at[g]))
        copies[-1].start()
    for copy in copies:
        copy.wait()


def analyse(blocks, total, pulled):
    cells, entries = total.shape
    members = len(blocks) * blocks[0].shape[0]
    return pl.pallas_call(
        analyse_kernel,
        out_shape=jax.ShapeDtypeStruct((entries, cells, members), jnp.float32),
        out_specs=pl.BlockSpec(memory_space=pl.ANY),
        scratch_shapes=[
            pltpu.VMEM((members * IN_STEP, entries), jnp.float32),
            pltpu.VMEM((entries * OUT_STEP, members), jnp.float32),
            pltpu.SemaphoreType.DMA((cells // (2 * GROUP),)),
        ],
        compiler_params=GRANT,
        name="analyse",
    )(blocks, total, pulled)


def neighbours(axis):
    up = [(i, i + 1) for i in range(lax.axis_size(axis) - 1)]
    return up, [(j, i) for i, j in up]


def body(
    background_sample,
    coupling,
    diffusion,
    wind_row,
    wind_col,
    observed_entry_index,
    obs_value,
    obs_weight,
):
    members_here, variables, levels, rows, cols = background_sample.shape
    entries = variables * levels
    dests = lax.axis_size("mem")
    own_w, own_e, *own = turn(background_sample)
    tops, bottoms = (own[0::2], own[1::2])
    col_up, col_down = neighbours("col")
    row_up, row_down = neighbours("row")
    west = lax.ppermute(own_e, "col", col_up)
    east = lax.ppermute(own_w, "col", col_down)
    norths = [lax.ppermute(bottoms[0], "row", row_up)]
    souths = [lax.ppermute(tops[0], "row", row_down)]
    sides = jnp.concatenate([west, east], axis=2)
    corner_n = lax.ppermute(sides[:, HALO:], "row", row_up)
    corner_s = lax.ppermute(sides[:, :HALO], "row", row_down)
    later = (tops[1:], bottoms[1:])
    later, west, east = lax.optimization_barrier((later, west, east))
    norths += [lax.ppermute(x, "row", row_up) for x in later[1]]
    souths += [lax.ppermute(x, "row", row_down) for x in later[0]]
    rates = jnp.concatenate(
        [
            jnp.stack([diffusion, wind_row, wind_col]),
            jnp.pad(coupling, ((0, 0), (0, levels - variables))),
        ]
    )
    moved = []
    for m in range(members_here):
        sent = forecast(
            m, dests, rates, tops[m], bottoms[m], norths[m], souths[m], west, east, corner_n, corner_s
        )
        moved.append(lax.all_to_all(sent, "mem", split_axis=0, concat_axis=0, tiled=True))
    cells = rows * cols // dests

    def listed(x):
        return jnp.transpose(x, (1, 2, 0)).reshape(cells, x.shape[0])

    total, pulled = weigh(
        listed(observed_entry_index), listed(obs_value), listed(obs_weight), entries
    )
    result = analyse(moved, total, pulled)
    result = result.reshape(variables, levels, rows, cols // dests, dests * members_here)
    return jnp.transpose(result, (4, 0, 1, 2, 3))


def solution(mesh):
    obs = P(None, "row", ("col", "mem"))

    return jax.shard_map(
        body,
        mesh=mesh,
        in_specs=(P("mem", None, None, "row", "col"), P(), P(), P(), P(), obs, obs, obs),
        out_specs=P(None, None, None, "row", ("col", "mem")),
        check_vma=False,
    )
```
